512 devices in a mesh: lat: 64 (over y_hi, x, z), ord: 8 (over y_lo, core).
Axes of the slice: x: 4, y: 8 (y_hi: 2, y_lo: 4; y = y_hi * 4 + y_lo), z: 8, core: 2. Of those that a mesh axis runs over, the one named last changes fastest.
Arguments:
- pressure: bfloat16 [2, 512, 5760], P(None, 'lat', 'ord'), may hold values from -6 to 6
- tables: bfloat16 [512, 512, 2048], P('ord', 'lat'), may hold values from -16 to 16
- quad_weight: float32 [512], replicated, may hold values from 0.5 to 2
- love_number: float32 [2048], replicated, may hold values from -0.5 to 0
- order_list: int32 [512], replicated, may hold values from 0 to 511, each once
- cycle_list: int32 [512], P('lat'), may hold values from 0 to 511, each once
Outputs:
- spectrum: float32 [2, 512, 2048], P(None, 'ord', 'lat')
- load_field: float32 [2, 512, 5760], P(None, 'lat', 'ord')
The draws below stay inside these ranges and needn't reach their ends.
Inputs may be any that keep to these rules, and one draw needn't show every extreme that they name: `order_list`: every order from 0 to 511 stands in exactly one slot. `cycle_list`: every northern cycle from 0 to 511 stands in exactly one slot; the same slot of the southern half holds its mirror cycle.
All inputs are finite; a program needn't handle non-finite values.
Results may differ from the reference program's by a relative error of at most 0.0055.
Values may be sent and summed in bfloat16 or wider, within the bound.
A program may use at most 64 MiB of HBM per device.

```python
import math
import jax
import jax.numpy as jnp
from jax import lax

NLON = 5760
LDEG = 2048
NORD = 512
NHALF = 512


def with_spikes(array, stream_key, source, target, blocks, factor):
    def block_of(dim):
        return (jnp.arange(array.shape[dim]) // (array.shape[dim] // blocks)).reshape((-1,) + (1,) * (array.ndim - 1 - dim))

    near = jax.random.permutation(stream_key, blocks)[block_of(target)]
    other_side = (block_of(target) + blocks // 2) % blocks
    return jnp.where((block_of(source) == near) | (block_of(source) == other_side), factor * array, array)


def levels(stream_key, extent, pieces, smallest, high):
    level, own = 1.0, jax.random.fold_in(stream_key, 6)
    for dim, blocks in pieces:
        draws = jnp.exp(jax.random.uniform(jax.random.fold_in(own, dim), (blocks,), jnp.float32, smallest / len(pieces), high / len(pieces)))
        level = level * jnp.repeat(draws, extent[dim] // blocks).reshape([-1 if axis == dim else 1 for axis in range(len(extent))])
    return level


def normal_values(own_key, dims, scale, limit, cuts=(), kind=jnp.bfloat16):
    result = jax.random.normal(own_key, dims, jnp.float32) * scale
    if len(cuts) > 0:
        result = levels(own_key, dims, cuts, -0.22, 0.18) * result
    return jnp.clip(result, min=-limit, max=limit).astype(kind)


def heavy_noise(own_key, extent, scale, reach, pieces, heavy, held_as=jnp.bfloat16):
    values = scale * jax.random.normal(own_key, extent, jnp.float32)
    if pieces:
        values = values * levels(own_key, extent, pieces, -0.22, 0.18)
    return jnp.clip(with_spikes(values, jax.random.fold_in(own_key, 3), *heavy), -reach, reach).astype(held_as)


def setup_inputs(seed: int = 0) -> dict:
    splits = jax.random.split(jax.random.key(seed), 7)
    return {
        "pressure": normal_values(splits[0], (2, NHALF, NLON), 1.0, 6.0, ((1, 64), (2, 8))),
        "tables": heavy_noise(splits[1], (NORD, NHALF, LDEG), 1.0, 16.0, ((0, 8), (1, 64)), (1, 2, 64, 4.0)),
        "quad_weight": jnp.clip(jnp.exp(jax.random.uniform(splits[2], (NHALF,), jnp.float32, math.log(0.5), math.log(2.0))), 0.5, 2.0),
        "love_number": jnp.clip(jax.random.uniform(splits[3], (LDEG,), jnp.float32, -0.5, 0.0), -0.5, 0.0),
        "order_list": jax.random.permutation(splits[4], NORD).astype(jnp.int32),
        "cycle_list": jax.random.permutation(splits[5], NHALF).astype(jnp.int32),
    }


DENSITY_RATIO = 3.0 * 1025.0 / 5517.0

def phase_table(order_values, positions):
    phase = order_values[:, None] * positions[None, :] % NLON
    angle = phase.astype(jnp.float32) * (2.0 * math.pi / NLON)
    return (jnp.cos(angle).astype(jnp.bfloat16), jnp.sin(angle).astype(jnp.bfloat16))

def reference(pressure, tables, quad_weight, love_number, order_list, cycle_list):
    grid_rows = pressure.reshape(2 * NHALF, NLON)
    cosine_table, sine_table = phase_table(order_list, jnp.arange(NLON, dtype=jnp.int32))
    lon_scale = 1.0 / math.sqrt(NLON)
    real_part = lon_scale * jnp.dot(grid_rows, cosine_table.T, preferred_element_type=jnp.float32)
    imag_part = -lon_scale * jnp.dot(grid_rows, sine_table.T, preferred_element_type=jnp.float32)
    cycle_weight = (quad_weight[cycle_list] * (1.0 / math.sqrt(NHALF)))[:, None]
    north_real = real_part[:NHALF]
    south_real = real_part[NHALF:]
    north_imag = imag_part[:NHALF]
    south_imag = imag_part[NHALF:]
    folded = jnp.stack([cycle_weight * (north_real + south_real), cycle_weight * (north_imag + south_imag), cycle_weight * (north_real - south_real), cycle_weight * (north_imag - south_imag)], 0)
    folded = jnp.transpose(folded.astype(jnp.bfloat16), (2, 1, 0))
    degree = jnp.arange(LDEG, dtype=jnp.int32)

    def analyse(item):
        table, column, order_value = item
        product = jnp.dot(column.T, table, preferred_element_type=jnp.float32)
        even = (degree + order_value) % 2 == 0
        present = degree >= order_value
        coeff_real = jnp.where(present, jnp.where(even, product[0], product[2]), 0.0)
        coeff_imag = jnp.where(present, jnp.where(even, product[1], product[3]), 0.0)
        return jnp.stack([coeff_real, coeff_imag], 0)
    coefficients = lax.map(analyse, (tables, folded, order_list))
    spectrum = jnp.transpose(coefficients, (1, 0, 2))
    love_factor = DENSITY_RATIO * (1.0 + love_number)
    scaled = (love_factor * coefficients).astype(jnp.bfloat16)
    deg_scale = 1.0 / math.sqrt(LDEG)

    def synthesise(item):
        table, coeff, order_value = item
        even = (degree + order_value) % 2 == 0
        zero = jnp.zeros_like(coeff[0])
        stacked = jnp.stack([jnp.where(even, coeff[0], zero), jnp.where(even, coeff[1], zero), jnp.where(even, zero, coeff[0]), jnp.where(even, zero, coeff[1])], 0)
        summed = jnp.dot(table, stacked.T, preferred_element_type=jnp.float32)
        north = deg_scale * (summed[:, :2] + summed[:, 2:])
        south = deg_scale * (summed[:, :2] - summed[:, 2:])
        return jnp.stack([north, south], 0).astype(jnp.bfloat16)
    synthesised = lax.map(synthesise, (tables, scaled, order_list))
    synth_real = synthesised[..., 0].reshape(NORD, 2 * NHALF)
    synth_imag = synthesised[..., 1].reshape(NORD, 2 * NHALF)
    field = jnp.dot(synth_real.T, cosine_table, preferred_element_type=jnp.float32) - jnp.dot(synth_imag.T, sine_table, preferred_element_type=jnp.float32)
    load_field = (1.0 / math.sqrt(NORD) * field).reshape(2, NHALF, NLON)
    return (spectrum, load_field)
```

```python
import functools
import math

import jax
import jax.numpy as jnp
from jax import lax
from jax.experimental import pallas as pl
from jax.experimental.pallas import tpu as pltpu
from jax.sharding import PartitionSpec as P

NLON = 5760
DENSITY_RATIO = 3.0 * 1025.0 / 5517.0
NY, NX, NZ = 2, 4, 8
LANES = 128
F32 = jnp.float32
BF16 = jnp.bfloat16


def dot(a, b, dims):
    return lax.dot_general(a, b, (dims, ((), ())), preferred_element_type=F32)


def turn(phase):
    quarter = NLON // 4
    q = jnp.floor(phase * (1.0 / quarter) + 0.5)
    x = (phase - q * quarter) * (2.0 * math.pi / NLON)
    q = q.astype(jnp.int32)
    z = x * x
    s = x + x * z * (-1.6666654611e-1 + z * (8.3321608736e-3 + z * -1.9515295891e-4))
    c = 1.0 - 0.5 * z + z * z * (4.166664568298827e-2 + z * (-1.388731625493765e-3 + z * 2.443315711809948e-5))
    odd = (q & 1) == 1
    cos = jnp.where(odd, s, c)
    sin = jnp.where(odd, c, s)
    cos = jnp.where(((q + 1) & 2) == 2, -cos, cos)
    return cos, jnp.where((q & 2) == 2, sin, -sin)


def kernel(
    sizes,
    p_ref,
    tab_hbm,
    qw_ref,
    love_ref,
    ord_ref,
    cyc_ref,
    spec_ref,
    field_ref,
    tab,
    trig,
    mcol,
    ptile,
    ssend,
    srecv,
    lhs,
    vbuf,
    xr,
    ubuf,
    zr,
    ysend,
    yr,
    coef,
    sgn,
    tab_sem,
    os_s,
    os_r,
    xs_s,
    xs_r,
    zs_s,
    zs_r,
    ys_s,
    ys_r,
    zg_s,
    zg_r,
    xg_s,
    xg_r,
    og_s,
    og_r,
):
    no, j, lon, ml, order_total, half_total, degrees = sizes
    rows = 2 * ml
    kk = ml * j
    run = degrees // (NY * NX)
    share = run // NZ
    blocks = -(-lon // LANES)
    lat = lax.axis_index("lat")
    me_o = lax.axis_index("ord")
    yh = lat // (NX * NZ)
    x = (lat // NZ) % NX
    z = lat % NZ

    def at(k_y, k_x, k_z):
        to = (((yh + k_y) % NY) * NX + (x + k_x) % NX) * NZ + (z + k_z) % NZ
        return {"lat": to}

    def send(src, dst, send_sem, recv_sem, device):
        copy = pltpu.make_async_remote_copy(
            src_ref=src,
            dst_ref=dst,
            send_sem=send_sem,
            recv_sem=recv_sem,
            device_id=device,
            device_id_type=pl.DeviceIdType.MESH,
        )
        copy.start()
        return copy

    peers = [{"ord": (me_o + k) % no} for k in range(1, no)]
    peers += [at(0, k, 0) for k in range(1, NX)]
    peers += [at(0, 0, k) for k in range(1, NZ)]
    peers += [at(1, 0, 0)]
    barrier = pltpu.get_barrier_semaphore()
    for peer in peers:
        pl.semaphore_signal(barrier, inc=1, device_id=peer, device_id_type=pl.DeviceIdType.MESH)

    tab_copy = pltpu.make_async_copy(tab_hbm, tab, tab_sem)
    tab_copy.start()

    width = ord_ref.shape[1]
    for g in range(ord_ref.shape[0]):
        line = ord_ref[g : g + 1, :].astype(F32)
        mcol[g * width : (g + 1) * width, :] = jnp.broadcast_to(line, (LANES, width)).T

    for h in range(2):
        ptile[h * j : (h + 1) * j, :] = jnp.zeros((j, blocks * LANES), F32)
        ptile[h * j : (h + 1) * j, :lon] = p_ref[h].astype(F32)
    grid_rows = ptile[...].astype(BF16)

    lane = lax.broadcasted_iota(jnp.int32, (8, LANES), 1).astype(F32)
    lon0 = (me_o * lon).astype(F32) + lane

    def make_group(g):
        m = mcol[pl.ds(pl.multiple_of(g * 8, 8), 8), :]
        c, s = turn(m * lon0)
        dc, ds = turn(m * float(LANES))
        at_row = pl.ds(pl.multiple_of(g * 16, 16), 16)
        for b in range(blocks):
            trig[at_row, b * LANES : (b + 1) * LANES] = jnp.concatenate([c, s], 0).astype(BF16)
            if b < blocks - 1:
                c, s = c * dc - s * ds, c * ds + s * dc

    ord_copies = []
    for k in [*range(1, no), 0]:
        to = (me_o + k) % no

        def two(i, carry, to=to):
            make_group(to * NZ + 2 * i)
            make_group(to * NZ + 2 * i + 1)
            return carry

        lax.fori_loop(0, NZ // 2, two, 0)
        part = dot(grid_rows, trig[pl.ds(pl.multiple_of(to * rows, rows), rows), :], ((1,), (1,)))
        if k == 0:
            own_part = part
            break
        ssend[k - 1] = part
        if k == 1:
            pl.semaphore_wait(barrier, len(peers))
        ord_copies.append(
            send(ssend.at[k - 1], srecv.at[k - 1], os_s.at[k - 1], os_r.at[k - 1], {"ord": to})
        )

    mloc = mcol[pl.ds(pl.multiple_of(me_o * ml, 8), ml), :]
    mrow = jnp.concatenate([mloc[8 * (i // 2) : 8 * (i // 2) + 8] for i in range(2 * NZ)], 0)
    mrow = jnp.concatenate([mrow] * (run // LANES), 1).astype(jnp.int32)
    run_lane = lax.broadcasted_iota(jnp.int32, (rows, run), 1)
    even = ((run_lane + mrow) & 1) == 0
    row_i = lax.broadcasted_iota(jnp.int32, (rows, kk), 0)
    col_i = lax.broadcasted_iota(jnp.int32, (rows, kk), 1)
    same_slot = (row_i // 16) * 8 + row_i % 8 == col_i // j
    pick_j = lax.broadcasted_iota(jnp.int32, (j, kk), 0)
    pick_c = lax.broadcasted_iota(jnp.int32, (j, kk), 1)
    pick = jnp.where(pick_j == pick_c % j, 1.0, 0.0).astype(BF16)

    row_j = lax.broadcasted_iota(jnp.int32, (j, rows), 0)
    weight = jnp.zeros((j, rows), F32)
    for i in range(j):
        weight = jnp.where(row_j == i, qw_ref[cyc_ref[i]], weight)
    weight = weight * (1.0 / math.sqrt(half_total))

    total = own_part
    for k in range(no - 1):
        ord_copies[k].wait_recv()
        total = total + srecv[k]
    total = total * (1.0 / math.sqrt(NLON))
    north, south = total[:j], total[j:]
    for i, folded in enumerate((weight * (north + south), weight * (north - south))):
        spread = dot(folded.T.astype(BF16), pick, ((1,), (0,)))
        lhs[i * rows : (i + 1) * rows, :] = jnp.where(same_slot, spread, 0.0).astype(BF16)

    tab_copy.wait()

    def degree_base(y, col):
        return pl.multiple_of(y * (NX * run) + col * run, run)

    def table_block(base):
        return tab[:, :, pl.ds(base, run)].reshape(kk, run)

    x_order = [2, 1, 3] if NX == 4 else [*range(1, NX)]
    z_order = sorted(range(1, NZ), key=lambda k: -min(k, NZ - k))
    x_copies = {}
    for kx in [*x_order, 0]:
        for y in range(NY):
            base = degree_base(y, (x + kx) % NX)
            prod = dot(lhs[...], table_block(base), ((1,), (0,)))
            value = jnp.where(even, prod[:rows], prod[rows:])
            value = jnp.where(run_lane + base >= mrow, value, 0.0)
            vbuf[kx, :, y * run : (y + 1) * run] = value.astype(BF16)
        if kx:
            for kz in [*z_order, 0]:
                piece = pl.ds(pl.multiple_of(((z + kz) % NZ) * 16, 16), 16)
                x_copies[kx, kz] = send(
                    vbuf.at[kx, piece],
                    xr.at[kx - 1, piece],
                    xs_s.at[kx - 1, kz],
                    xs_r.at[kx - 1, kz],
                    at(0, kx, 0),
                )

    z_copies = {}
    for kz in [*z_order, 0]:
        piece = pl.ds(pl.multiple_of(((z + kz) % NZ) * 16, 16), 16)
        summed = vbuf[0, piece, :].astype(F32)
        for kx in range(1, NX):
            x_copies[kx, kz].wait_recv()
            summed = summed + xr[kx - 1, piece, :].astype(F32)
        if kz:
            ubuf[kz - 1] = summed.astype(BF16)
            z_copies[kz] = send(
                ubuf.at[kz - 1], zr.at[kz - 1], zs_s.at[kz - 1], zs_r.at[kz - 1], at(0, 0, kz)
            )
    for kz in range(1, NZ):
        z_copies[kz].wait_recv()
        summed = summed + zr[kz - 1].astype(F32)
    ysend[...] = summed.astype(BF16)
    y_copy = send(ysend, yr, ys_s, ys_r, at(1, 0, 0))
    love = jnp.concatenate(
        [
            love_ref[pl.ds((y * NX * run + x * run) // LANES + i, 1), :]
            for y in range(NY)
            for i in range(run // LANES)
        ],
        1,
    )
    factor = DENSITY_RATIO * (1.0 + love)
    y_copy.wait_recv()
    summed = summed + yr[...].astype(F32)
    own_piece = pl.ds(pl.multiple_of(z * 16, 16), 16)
    coef[0, own_piece, :] = (factor * summed).astype(BF16)

    g_copies = []
    zg_copies = {}
    for kz in z_order:
        zg_copies[kz] = send(
            coef.at[0, own_piece], coef.at[0, own_piece], zg_s.at[kz - 1], zg_r.at[kz - 1], at(0, 0, kz)
        )
    for kz in [0, *reversed(z_order)]:
        piece = pl.ds(pl.multiple_of(((z + NZ - kz) % NZ) * 16, 16), 16)
        if kz:
            zg_copies[kz].wait_recv()
        for kx in x_order:
            g_copies.append(
                (
                    kx,
                    send(
                        coef.at[0, piece],
                        coef.at[kx, piece],
                        xg_s.at[kx - 1, kz],
                        xg_r.at[kx - 1, kz],
                        at(0, kx, 0),
                    ),
                )
            )

    synth = jnp.zeros((2 * rows, kk), F32)
    for kx in [0, *reversed(x_order)]:
        for k, copy in g_copies:
            if k == kx:
                copy.wait_recv()
        for y in range(NY):
            base = degree_base(y, (x + NX - kx) % NX)
            block = coef[kx, :, y * run : (y + 1) * run].astype(F32)
            both = jnp.concatenate([block, jnp.where(even, block, -block)], 0).astype(BF16)
            synth = synth + dot(both, table_block(base), ((1,), (1,)))

    halves = []
    for h in range(2):
        part = jnp.where(same_slot, synth[h * rows : (h + 1) * rows] * (1.0 / math.sqrt(degrees)), 0.0)
        halves.append(dot(pick, part.astype(BF16), ((1,), (1,))))
    sgn[0] = jnp.concatenate(halves, 0).astype(BF16)
    og_copies = [
        send(sgn.at[0], sgn.at[k], og_s.at[k - 1], og_r.at[k - 1], {"ord": (me_o + k) % no})
        for k in range(1, no)
    ]

    mine = coef[0, :, pl.ds(pl.multiple_of(yh * run, run), run)]
    sel_i = lax.broadcasted_iota(jnp.int32, (run, share), 0)
    sel_o = lax.broadcasted_iota(jnp.int32, (run, share), 1)
    sel = jnp.where(sel_i == sel_o + z * share, 1.0, 0.0)
    out = dot(mine, sel.astype(BF16), ((1,), (0,)))
    first = (yh * NX * run + x * run) // LANES
    love_run = jnp.concatenate([love_ref[pl.ds(first + i, 1), :] for i in range(run // LANES)], 1)
    own_factor = jnp.sum(jnp.where(sel > 0.5, (DENSITY_RATIO * (1.0 + love_run)).T, 0.0), 0, keepdims=True)
    out = out / own_factor
    for i in range(NZ):
        for c in range(2):
            spec_ref[c, i * 8 : (i + 1) * 8, :] = out[i * 16 + c * 8 : i * 16 + c * 8 + 8]

    field = jnp.zeros((2 * j, blocks * LANES), F32)
    for k in range(no):
        if k:
            og_copies[k - 1].wait_recv()
        source = (me_o + no - k) % no
        rows_of = pl.ds(pl.multiple_of(source * rows, rows), rows)
        field = field + dot(sgn[k], trig[rows_of, :], ((1,), (0,)))
    field = field * (1.0 / math.sqrt(order_total))
    for h in range(2):
        field_ref[h] = field[h * j : (h + 1) * j, :lon]

    for copy in [*ord_copies, *x_copies.values(), *z_copies.values(), y_copy, *zg_copies.values(), *og_copies]:
        copy.wait_send()
    for _, copy in g_copies:
        copy.wait_send()


def per_device(no, pressure, tables, quad_weight, love_number, order_list, cycle_list):
    j, lon = pressure.shape[1:]
    ml, _, degrees = tables.shape
    order_total = order_list.shape[0]
    rows = 2 * ml
    run = degrees // (NY * NX)
    lon_pad = -(-lon // LANES) * LANES
    width = min(LANES, order_total)
    sizes = (no, j, lon, ml, order_total, quad_weight.shape[0], degrees)
    vmem = pl.BlockSpec(memory_space=pltpu.VMEM)
    smem = pl.BlockSpec(memory_space=pltpu.SMEM)
    dma = pltpu.SemaphoreType.DMA
    spectrum, field = pl.pallas_call(
        functools.partial(kernel, sizes),
        out_shape=(
            jax.ShapeDtypeStruct((2, ml, run // NZ), F32),
            jax.ShapeDtypeStruct((2, j, lon), F32),
        ),
        in_specs=[vmem, pl.BlockSpec(memory_space=pl.ANY), smem, vmem, vmem, smem],
        out_specs=(vmem, vmem),
        scratch_shapes=[
            pltpu.VMEM((ml, j, degrees), BF16),
            pltpu.VMEM((no * rows, lon_pad), BF16),
            pltpu.VMEM((order_total, LANES), F32),
            pltpu.VMEM((2 * j, lon_pad), F32),
            pltpu.VMEM((no - 1, 2 * j, rows), F32),
            pltpu.VMEM((no - 1, 2 * j, rows), F32),
            pltpu.VMEM((2 * rows, ml * j), BF16),
            pltpu.VMEM((NX, rows, NY * run), BF16),
            pltpu.VMEM((NX - 1, rows, NY * run), BF16),
            pltpu.VMEM((NZ - 1, 16, NY * run), BF16),
            pltpu.VMEM((NZ - 1, 16, NY * run), BF16),
            pltpu.VMEM((16, NY * run), BF16),
            pltpu.VMEM((16, NY * run), BF16),
            pltpu.VMEM((NX, rows, NY * run), BF16),
            pltpu.VMEM((no, 2 * j, rows), BF16),
            dma,
            dma((no - 1,)),
            dma((no - 1,)),
            dma((NX - 1, NZ)),
            dma((NX - 1, NZ)),
            dma((NZ - 1,)),
            dma((NZ - 1,)),
            dma,
            dma,
            dma((NZ - 1,)),
            dma((NZ - 1,)),
            dma((NX - 1, NZ)),
            dma((NX - 1, NZ)),
            dma((no - 1,)),
            dma((no - 1,)),
        ],
        compiler_params=pltpu.CompilerParams(collective_id=0, has_side_effects=True),
        name="load_step",
    )(
        pressure,
        tables,
        quad_weight,
        love_number.reshape(-1, LANES),
        order_list.reshape(-1, width),
        cycle_list,
    )
    return spectrum, field


def solution(mesh):
    placed = (P(None, "lat", "ord"), P("ord", "lat", None), P(), P(), P(), P("lat"))
    return jax.shard_map(
        functools.partial(per_device, mesh.shape["ord"]),
        mesh=mesh,
        in_specs=placed,
        out_specs=(P(None, "ord", "lat"), P(None, "lat", "ord")),
        check_vma=False,
    )
```

```python
import functools
import math

import jax
import jax.numpy as jnp
from jax import lax
from jax.experimental import pallas as pl
from jax.experimental.pallas import tpu as pltpu
from jax.sharding import PartitionSpec as P

NLON = 5760
DENSITY_RATIO = 3.0 * 1025.0 / 5517.0
NY, NX, NZ = 2, 4, 8
LANES = 128
F32 = jnp.float32
BF16 = jnp.bfloat16


def dot(a, b, dims):
    return lax.dot_general(a, b, (dims, ((), ())), preferred_element_type=F32)


def turn(phase):
    quarter = NLON // 4
    q = jnp.floor(phase * (1.0 / quarter) + 0.5)
    x = (phase - q * quarter) * (2.0 * math.pi / NLON)
    q = q.astype(jnp.int32)
    z = x * x
    s = x + x * z * (-1.6666654611e-1 + z * (8.3321608736e-3 + z * -1.9515295891e-4))
    c = 1.0 - 0.5 * z + z * z * (4.166664568298827e-2 + z * (-1.388731625493765e-3 + z * 2.443315711809948e-5))
    odd = (q & 1) == 1
    cos = jnp.where(odd, s, c)
    sin = jnp.where(odd, c, s)
    cos = jnp.where(((q + 1) & 2) == 2, -cos, cos)
    return cos, jnp.where((q & 2) == 2, sin, -sin)


def kernel(
    sizes,
    p_hbm,
    tab_hbm,
    qw_hbm,
    love_hbm,
    ord_hbm,
    cyc_hbm,
    spec_ref,
    field_ref,
    p_ref,
    qw_ref,
    love_ref,
    ord_ref,
    cyc_ref,
    tab,
    trig,
    base,
    mcol,
    ptile,
    ssend,
    srecv,
    lhs,
    vbuf,
    xr,
    ubuf,
    zr,
    ysend,
    yr,
    coef,
    sgn,
    in_sem,
    os_s,
    os_r,
    xs_s,
    xs_r,
    zs_s,
    zs_r,
    ys_s,
    ys_r,
    zg_s,
    zg_r,
    xg_s,
    xg_r,
    og_s,
    og_r,
):
    no, j, lon, ml, order_total, half_total, degrees = sizes
    rows = 2 * ml
    kk = ml * j
    run = degrees // (NY * NX)
    share = run // NZ
    blocks = -(-lon // LANES)
    lat = lax.axis_index("lat")
    me_o = lax.axis_index("ord")
    yh = lat // (NX * NZ)
    x = (lat // NZ) % NX
    z = lat % NZ

    def at(k_y, k_x, k_z):
        to = (((yh + k_y) % NY) * NX + (x + k_x) % NX) * NZ + (z + k_z) % NZ
        return {"lat": to}

    def send(src, dst, send_sem, recv_sem, device):
        copy = pltpu.make_async_remote_copy(
            src_ref=src,
            dst_ref=dst,
            send_sem=send_sem,
            recv_sem=recv_sem,
            device_id=device,
            device_id_type=pl.DeviceIdType.MESH,
        )
        copy.start()
        return copy

    loads = {}
    for i, (name, src, dst) in enumerate(
        (
            ("ord", ord_hbm, ord_ref),
            ("p", p_hbm, p_ref),
            ("cyc", cyc_hbm, cyc_ref),
            ("qw", qw_hbm, qw_ref),
            ("love", love_hbm, love_ref),
            ("tab", tab_hbm, tab),
        )
    ):
        loads[name] = pltpu.make_async_copy(src, dst, in_sem.at[i])
        loads[name].start()

    peers = [{"ord": (me_o + k) % no} for k in range(1, no)]
    peers += [at(0, k, 0) for k in range(1, NX)]
    peers += [at(0, 0, k) for k in range(1, NZ)]
    peers += [at(1, 0, 0)]
    barrier = pltpu.get_barrier_semaphore()
    for peer in peers:
        pl.semaphore_signal(barrier, inc=1, device_id=peer, device_id_type=pl.DeviceIdType.MESH)

    loads["ord"].wait()
    order_f = ord_ref[...].astype(F32)
    width = order_f.shape[1]
    lines = [order_f[g : g + 1] for g in range(order_f.shape[0])]
    for g, line in enumerate(lines):
        mcol[g * width : (g + 1) * width, :] = jnp.broadcast_to(line, (LANES, width)).T
    m_lanes = jnp.concatenate(lines, 1)

    lane = lax.broadcasted_iota(jnp.int32, (16, LANES), 1).astype(F32)

    def make_base(g, carry):
        at_row = pl.multiple_of(g * 16, 16)
        for i, part in enumerate(turn(mcol[pl.ds(at_row, 16), :] * lane)):
            high = part.astype(BF16)
            base[pl.ds(i * order_total + at_row, 16), :LANES] = high
            base[pl.ds(i * order_total + at_row, 16), LANES:] = (part - high.astype(F32)).astype(BF16)
        return carry

    lax.fori_loop(0, order_total // 16, make_base, 0, unroll=4)

    loads["p"].wait()
    ptile[...] = jnp.zeros_like(ptile)
    for h in range(2):
        ptile[h * j : (h + 1) * j, :lon] = p_ref[h].astype(F32)
    split = jnp.concatenate([ptile[:, b * LANES : (b + 1) * LANES] for b in range(blocks)], 0)
    split = jnp.concatenate([split, split], 1).astype(BF16)
    first = dot(split, base[...], ((1,), (1,)))
    start = (lax.broadcasted_iota(jnp.int32, (blocks, order_total), 0) * LANES + me_o * lon).astype(F32)
    tc, ts = turn(m_lanes * start)
    re = im = 0.0
    for b in range(blocks):
        c = first[b * 2 * j : (b + 1) * 2 * j, :order_total]
        s = first[b * 2 * j : (b + 1) * 2 * j, order_total:]
        re = re + c * tc[b : b + 1] - s * ts[b : b + 1]
        im = im + c * ts[b : b + 1] + s * tc[b : b + 1]
    for d in range(no):
        cols = slice(d * ml, (d + 1) * ml)
        ssend[d] = jnp.concatenate([re[:, cols], im[:, cols]], 1)
    pl.semaphore_wait(barrier, len(peers))
    ord_copies = []
    for k in [*range(no // 2, no), *range(1, no // 2)]:
        to = (me_o + k) % no
        ord_copies.append(send(ssend.at[to], srecv.at[k - 1], os_s.at[k - 1], os_r.at[k - 1], {"ord": to}))

    lane8 = lax.broadcasted_iota(jnp.int32, (8, LANES), 1).astype(F32)
    lon0 = (me_o * lon).astype(F32) + lane8

    def make_group(g, carry):
        m = mcol[pl.ds(pl.multiple_of(g * 8, 8), 8), :]
        c, s = turn(m * lon0)
        dc, ds = turn(m * float(LANES))
        at_row = pl.ds(pl.multiple_of(g * 16, 16), 16)
        for b in range(blocks):
            trig[at_row, b * LANES : (b + 1) * LANES] = jnp.concatenate([c, s], 0).astype(BF16)
            if b < blocks - 1:
                c, s = c * dc - s * ds, c * ds + s * dc
        return carry

    lax.fori_loop(0, order_total // 8, make_group, 0, unroll=4)

    mloc = mcol[pl.ds(pl.multiple_of(me_o * ml, 8), ml), :]
    mrow = jnp.concatenate([mloc[8 * (i // 2) : 8 * (i // 2) + 8] for i in range(2 * NZ)], 0)
    mrow = jnp.concatenate([mrow] * (run // LANES), 1).astype(jnp.int32)
    run_lane = lax.broadcasted_iota(jnp.int32, (rows, run), 1)
    even = ((run_lane + mrow) & 1) == 0
    wide = NX * run
    wide_lane = lax.broadcasted_iota(jnp.int32, (8, wide), 1)
    row_i = lax.broadcasted_iota(jnp.int32, (rows, kk), 0)
    col_i = lax.broadcasted_iota(jnp.int32, (rows, kk), 1)
    same_slot = (row_i // 16) * 8 + row_i % 8 == col_i // j
    pick_j = lax.broadcasted_iota(jnp.int32, (j, kk), 0)
    pick_c = lax.broadcasted_iota(jnp.int32, (j, kk), 1)
    pick = jnp.where(pick_j == pick_c % j, 1.0, 0.0).astype(BF16)
    row_8 = lax.broadcasted_iota(jnp.int32, (rows, 8 * j), 0)
    col_8 = lax.broadcasted_iota(jnp.int32, (rows, 8 * j), 1)
    in_piece = row_8 % 8 == col_8 // j

    loads["cyc"].wait()
    loads["qw"].wait()
    row_j = lax.broadcasted_iota(jnp.int32, (j, rows), 0)
    weight = jnp.zeros((j, rows), F32)
    for i in range(j):
        weight = jnp.where(row_j == i, qw_ref[cyc_ref[i]], weight)
    weight = weight * (1.0 / math.sqrt(half_total))
    loads["love"].wait()
    loads["tab"].wait()

    total = ssend[me_o]
    for copy in ord_copies:
        copy.wait_recv()
    for k in range(no - 1):
        total = total + srecv[k]
    total = total * (1.0 / math.sqrt(NLON))
    north, south = total[:j], total[j:]
    for i, folded in enumerate((weight * (north + south), weight * (north - south))):
        spread = dot(folded.T.astype(BF16), pick[:, : 8 * j], ((1,), (0,)))
        spread = jnp.where(in_piece, spread, 0.0)
        for p in range(NZ):
            for c in range(2):
                lhs[p, (2 * i + c) * 8 : (2 * i + c) * 8 + 8, :] = spread[c * ml + p * 8 : c * ml + p * 8 + 8]

    x_order = [2, 1, 3] if NX == 4 else [*range(1, NX)]
    z_order = sorted(range(1, NZ), key=lambda k: -min(k, NZ - k))
    x_copies = {}
    for kz in [*z_order, 0]:
        zz = (z + kz) % NZ
        weights = lhs[zz].astype(BF16)
        m8 = mcol[pl.ds(pl.multiple_of(me_o * ml + zz * 8, 8), 8), :]
        m8 = jnp.concatenate([m8] * (wide // LANES), 1).astype(jnp.int32)
        even8 = ((wide_lane + m8) & 1) == 0
        for y in range(NY):
            block = tab[pl.ds(zz * 8, 8), :, y * wide : (y + 1) * wide].reshape(8 * j, wide)
            prod = dot(weights, block, ((1,), (0,)))
            present = wide_lane + y * wide >= m8
            value = [
                jnp.where(present, jnp.where(even8, prod[c * 8 : c * 8 + 8], prod[c * 8 + 16 : c * 8 + 24]), 0.0)
                for c in range(2)
            ]
            vbuf[kz, y] = jnp.concatenate(value, 0).astype(BF16)
        for kx in x_order:
            cols = pl.ds(pl.multiple_of(((x + kx) % NX) * run, run), run)
            x_copies[kx, kz] = send(
                vbuf.at[kz, :, :, cols],
                xr.at[kx - 1, kz],
                xs_s.at[kx - 1, kz],
                xs_r.at[kx - 1, kz],
                at(0, kx, 0),
            )

    own_cols = pl.ds(pl.multiple_of(x * run, run), run)
    z_copies = {}
    for kz in [*z_order, 0]:
        summed = vbuf[kz, :, :, own_cols].astype(F32)
        for kx in x_order:
            x_copies[kx, kz].wait_recv()
            summed = summed + xr[kx - 1, kz].astype(F32)
        if kz:
            ubuf[kz - 1] = summed.astype(BF16)
            z_copies[kz] = send(
                ubuf.at[kz - 1], zr.at[kz - 1], zs_s.at[kz - 1], zs_r.at[kz - 1], at(0, 0, kz)
            )
    for kz in z_order:
        z_copies[kz].wait_recv()
        summed = summed + zr[kz - 1].astype(F32)
    ysend[...] = summed.astype(BF16)
    y_copy = send(ysend, yr, ys_s, ys_r, at(1, 0, 0))
    def factor_of(y):
        at_love = (y * wide + x * run) // LANES
        return 1.0 + jnp.concatenate([love_ref[pl.ds(at_love + i, 1), :] for i in range(run // LANES)], 1)

    factors = [factor_of(y) for y in range(NY)]
    y_copy.wait_recv()
    summed = summed + yr[...].astype(F32)
    own_piece = pl.ds(pl.multiple_of(z * 16, 16), 16)
    for y in range(NY):
        coef[0, own_piece, y * run : (y + 1) * run] = (DENSITY_RATIO * factors[y] * summed[y]).astype(BF16)

    g_copies = []
    zg_copies = {}
    for kz in z_order:
        zg_copies[kz] = send(
            coef.at[0, own_piece], coef.at[0, own_piece], zg_s.at[kz - 1], zg_r.at[kz - 1], at(0, 0, kz)
        )
    for kz in [0, *reversed(z_order)]:
        piece = pl.ds(pl.multiple_of(((z + NZ - kz) % NZ) * 16, 16), 16)
        if kz:
            zg_copies[kz].wait_recv()
        for kx in x_order:
            g_copies.append(
                (
                    kx,
                    send(
                        coef.at[0, piece],
                        coef.at[kx, piece],
                        xg_s.at[kx - 1, kz],
                        xg_r.at[kx - 1, kz],
                        at(0, kx, 0),
                    ),
                )
            )

    synth = jnp.zeros((2 * rows, kk), F32)
    for kx in [0, *reversed(x_order)]:
        for k, copy in g_copies:
            if k == kx:
                copy.wait_recv()
        for y in range(NY):
            at_degree = pl.multiple_of(y * wide + ((x + NX - kx) % NX) * run, run)
            block = coef[kx, :, y * run : (y + 1) * run].astype(F32)
            both = jnp.concatenate([block, jnp.where(even, block, -block)], 0).astype(BF16)
            synth = synth + dot(both, tab[:, :, pl.ds(at_degree, run)].reshape(kk, run), ((1,), (1,)))

    halves = []
    for h in range(2):
        part = jnp.where(same_slot, synth[h * rows : (h + 1) * rows] * (1.0 / math.sqrt(degrees)), 0.0)
        halves.append(dot(pick, part.astype(BF16), ((1,), (1,))))
    sgn[0] = jnp.concatenate(halves, 0).astype(BF16)
    og_copies = [
        send(sgn.at[0], sgn.at[k], og_s.at[k - 1], og_r.at[k - 1], {"ord": (me_o + k) % no})
        for k in range(1, no)
    ]

    mine = coef[0, :, pl.ds(pl.multiple_of(yh * run, run), run)]
    sel_o = lax.broadcasted_iota(jnp.int32, (share, run), 0)
    sel_i = lax.broadcasted_iota(jnp.int32, (share, run), 1)
    sel = jnp.where(sel_i == sel_o + z * share, 1.0, 0.0)
    own_factor = jnp.sum(sel * factor_of(yh), 1, keepdims=True)
    out = dot(sel.astype(BF16), mine, ((1,), (1,))).astype(BF16)
    old = lax.broadcasted_iota(jnp.int32, (rows, rows), 0)
    new = lax.broadcasted_iota(jnp.int32, (rows, rows), 1)
    swap = old == ((new % ml) // 8) * 16 + (new // ml) * 8 + new % 8
    out = dot(out, jnp.where(swap, 1.0, 0.0).astype(BF16), ((1,), (0,)))
    out = out / own_factor
    for c in range(2):
        spec_ref[c] = out[:, c * ml : (c + 1) * ml]

    field = jnp.zeros((2 * j, blocks * LANES), F32)
    for k in range(no):
        if k:
            og_copies[k - 1].wait_recv()
        source = (me_o + no - k) % no
        rows_of = pl.ds(pl.multiple_of(source * rows, rows), rows)
        field = field + dot(sgn[k], trig[rows_of, :], ((1,), (0,)))
    for h in range(2):
        field_ref[h] = field[h * j : (h + 1) * j, :lon]

    for copy in [*ord_copies, *x_copies.values(), *z_copies.values(), y_copy, *zg_copies.values(), *og_copies]:
        copy.wait_send()
    for _, copy in g_copies:
        copy.wait_send()


def per_device(no, pressure, tables, quad_weight, love_number, order_list, cycle_list):
    j, lon = pressure.shape[1:]
    ml, _, degrees = tables.shape
    order_total = order_list.shape[0]
    rows = 2 * ml
    run = degrees // (NY * NX)
    share = run // NZ
    blocks = -(-lon // LANES)
    lon_pad = blocks * LANES
    width = min(LANES, order_total)
    sizes = (no, j, lon, ml, order_total, quad_weight.shape[0], degrees)
    vmem = pl.BlockSpec(memory_space=pltpu.VMEM)
    hbm = pl.BlockSpec(memory_space=pltpu.HBM)
    dma = pltpu.SemaphoreType.DMA
    spectrum, field = pl.pallas_call(
        functools.partial(kernel, sizes),
        out_shape=(
            jax.ShapeDtypeStruct((2, share, ml), F32),
            jax.ShapeDtypeStruct((2, j, lon), F32),
        ),
        in_specs=[hbm] * 6,
        out_specs=(vmem, vmem),
        scratch_shapes=[
            pltpu.VMEM((2, j, lon), BF16),
            pltpu.SMEM(quad_weight.shape, F32),
            pltpu.VMEM((degrees // LANES, LANES), F32),
            pltpu.VMEM((order_total // width, width), jnp.int32),
            pltpu.SMEM(cycle_list.shape, jnp.int32),
            pltpu.VMEM((ml, j, degrees), BF16),
            pltpu.VMEM((no * rows, lon_pad), BF16),
            pltpu.VMEM((2 * order_total, 2 * LANES), BF16),
            pltpu.VMEM((order_total, LANES), F32),
            pltpu.VMEM((2 * j, lon_pad), F32),
            pltpu.VMEM((no, 2 * j, rows), F32),
            pltpu.VMEM((no - 1, 2 * j, rows), F32),
            pltpu.VMEM((NZ, 32, 8 * j), F32),
            pltpu.VMEM((NZ, NY, 16, NX * run), BF16),
            pltpu.VMEM((NX - 1, NZ, NY, 16, run), BF16),
            pltpu.VMEM((NZ - 1, NY, 16, run), BF16),
            pltpu.VMEM((NZ - 1, NY, 16, run), BF16),
            pltpu.VMEM((NY, 16, run), BF16),
            pltpu.VMEM((NY, 16, run), BF16),
            pltpu.VMEM((NX, rows, NY * run), BF16),
            pltpu.VMEM((no, 2 * j, rows), BF16),
            dma((6,)),
            dma((no - 1,)),
            dma((no - 1,)),
            dma((NX - 1, NZ)),
            dma((NX - 1, NZ)),
            dma((NZ - 1,)),
            dma((NZ - 1,)),
            dma,
            dma,
            dma((NZ - 1,)),
            dma((NZ - 1,)),
            dma((NX - 1, NZ)),
            dma((NX - 1, NZ)),
            dma((no - 1,)),
            dma((no - 1,)),
        ],
        compiler_params=pltpu.CompilerParams(
            collective_id=0, has_side_effects=True, vmem_limit_bytes=24 * 1024 * 1024
        ),
        name="load_step",
    )(
        *(
            pltpu.with_memory_space_constraint(v, pltpu.HBM)
            for v in (
                pressure,
                tables,
                quad_weight,
                love_number.reshape(-1, LANES),
                order_list.reshape(-1, width),
                cycle_list,
            )
        )
    )
    return (jnp.swapaxes((1.0 / DENSITY_RATIO) * spectrum, 1, 2), (1.0 / math.sqrt(order_total)) * field)


def solution(mesh):
    placed = (P(None, "lat", "ord"), P("ord", "lat", None), P(), P(), P(), P("lat"))
    return jax.shard_map(
        functools.partial(per_device, mesh.shape["ord"]),
        mesh=mesh,
        in_specs=placed,
        out_specs=(P(None, "ord", "lat"), P(None, "lat", "ord")),
        check_vma=False,
    )
```
